512 devices in a mesh: groups: 2 (over y), tok: 16 (over z), head: 8 (over x), row: 2 (over core).
Axes of the slice: x: 8, y: 2, z: 16, core: 2. Of those that a mesh axis runs over, the one named last changes fastest.
The devices are a block of a 8x16x16 slice.
Arguments:
- text: bfloat16 [1024, 8192], P(('groups', 'row'), 'tok'), parts along dimension 0, may hold values from -12 to 12
- q_weight: bfloat16 [8192, 8192], P('tok', 'head'), may hold values from -0.0625 to 0.0625
- out_weight: bfloat16 [8192, 8192], P('head', 'tok'), may hold values from -0.0625 to 0.0625
- keys: bfloat16 [131072, 1024], P(('groups', 'tok'), 'head'), parts along dimension 0, may hold values from -60 to 60
- values: bfloat16 [131072, 1024], P(('groups', 'tok'), 'head'), parts along dimension 0, may hold values from -6 to 6
- gate: float32 [1], replicated, may hold values from 0.3 to 1.5
Outputs:
- result: bfloat16 [1024, 8192], P(('groups', 'row'), 'tok'), parts along dimension 0
The draws below stay inside these ranges and needn't reach their ends.
There are 2 independent parts, one for each index of `groups`. The reference program is written for one: setup_inputs(seed, part) draws one part's arguments, and reference() takes and returns one part's arrays. A program takes and returns all parts, laid end to end along the dimension named above; an argument that names none is the same for every part. Nothing has to cross between parts.
All inputs are finite; a program needn't handle non-finite values.
Results may differ from the reference program's by a relative error of at most 0.015.
Values may be sent and summed in bfloat16 or wider, within the bound.
A program may use at most 64 MiB of HBM per device.

```python
import jax
import jax.numpy as jnp
from jax import lax

D = 8192
HEADS = 64
KV = 8
HD = 128
GROUP = 8
TEXT = 512
VISUAL = 65536


def draw_text(key, part):
    first, second = jax.random.split(jax.random.fold_in(key, 11), 2)
    columns = 0.6 * 3.0 ** (jnp.arange(D, dtype=jnp.float32) / (D - 1))
    columns = columns * jnp.exp(jax.random.uniform(second, (D,), jnp.float32, 0.0, 0.7))
    base = jax.random.normal(first, (TEXT, D), jnp.float32)
    return jnp.clip(base * columns[None, :], -12.0, 12.0).astype(jnp.bfloat16)


def draw_keys(key, part):
    first = jax.random.fold_in(jax.random.fold_in(key, 23), 0)
    width = KV * HD
    base = jnp.clip(3.0 * jax.random.normal(first, (VISUAL, width), jnp.float32), -15.0, 15.0)
    return base.astype(jnp.bfloat16)


def block_levels(own_key, dims, shards, smallest, top_value):
    def one(dim, blocks):
        heights = jax.random.uniform(jax.random.fold_in(jax.random.fold_in(own_key, 6), dim), (blocks,), jnp.float32, smallest / len(shards), top_value / len(shards))
        return jnp.repeat(jnp.exp(heights), dims[dim] // blocks).reshape((-1,) + (1,) * (len(dims) - dim - 1))

    gain = one(*shards[0])
    for cut in shards[1:]:
        gain = gain * one(*cut)
    return gain


def centred(rng, extent, spread, most, shards=(), kind=jnp.bfloat16):
    values = jax.random.normal(rng, extent, jnp.float32) * spread
    if len(shards) > 0:
        values = block_levels(rng, extent, shards, -0.22, 0.18) * values
    return jnp.clip(values, min=-most, max=most).astype(kind)


def setup_inputs(seed: int = 0, part: int = 0) -> dict:
    seeds = jax.random.split(jax.random.key(seed), 7)
    own_keys = jax.random.split(jax.random.fold_in(seeds[6], part), 7)
    text = draw_text(jax.random.fold_in(jax.random.fold_in(seeds[6], part), 71), part)
    q_weight = centred(seeds[1], (D, HEADS * HD), D ** -0.5, 0.0625, ((0, 16), (1, 8)))
    out_weight = centred(seeds[2], (HEADS * HD, D), (HEADS * HD) ** -0.5, 0.0625, ((0, 8), (1, 16)))
    keys = draw_keys(jax.random.fold_in(jax.random.fold_in(seeds[6], part), 71), part)
    values = centred(own_keys[4], (VISUAL, KV * HD), 1.0, 6.0, ((0, 16), (1, 8)))
    gate = jnp.clip(jax.random.uniform(seeds[5], (1,), jnp.float32, 0.3, 1.5), 0.3, 1.5)
    return dict(text=text, q_weight=q_weight, out_weight=out_weight, keys=keys, values=values, gate=gate)


def reference(text, q_weight, out_weight, keys, values, gate):
    hidden = text.astype(jnp.float32)
    scale = lax.rsqrt(lax.optimization_barrier(jnp.mean(hidden * hidden, axis=1, keepdims=True)) + 1e-05)
    normed = (hidden * scale).astype(jnp.bfloat16)
    projected = jnp.dot(normed, q_weight, preferred_element_type=jnp.float32)
    rows = projected.shape[0]
    heads_view = projected.reshape(rows, KV, GROUP, HD)
    queries = (heads_view / jnp.sqrt(jnp.float32(HD))).astype(jnp.bfloat16)
    block = 2048 if VISUAL % 2048 == 0 else VISUAL
    count = VISUAL // block
    key_blocks = keys.reshape(count, block, KV, HD)
    value_blocks = values.reshape(count, block, KV, HD)
    query_float = queries.astype(jnp.float32)

    def step(carry, pair):
        running, total, accum = carry
        key_block, value_block = pair
        scores = jnp.einsum('tkgd,skd->ktgs', query_float, key_block.astype(jnp.float32))
        newmax = jnp.maximum(running, lax.optimization_barrier(jnp.max(scores, axis=3)))
        weights = jnp.exp(scores - newmax[..., None])
        factor = jnp.exp(running - newmax)
        total = total * factor + lax.optimization_barrier(jnp.sum(weights, axis=3))
        rounded = weights.astype(jnp.bfloat16).astype(jnp.float32)
        accum = accum * factor[..., None] + jnp.einsum('ktgs,skd->ktgd', rounded, value_block.astype(jnp.float32))
        return ((newmax, total, accum), None)
    start = (jnp.full((KV, rows, GROUP), -1e+30, jnp.float32), jnp.zeros((KV, rows, GROUP), jnp.float32), jnp.zeros((KV, rows, GROUP, HD), jnp.float32))
    (running, total, accum), _ = lax.scan(step, start, (key_blocks, value_blocks))
    outputs = accum / total[..., None]
    attended = jnp.transpose(outputs, (1, 0, 2, 3)).reshape(rows, HEADS * HD).astype(jnp.bfloat16)
    branch = jnp.dot(attended, out_weight, preferred_element_type=jnp.float32)
    return (hidden + jnp.tanh(gate[0]) * branch).astype(jnp.bfloat16)
```

```python
import functools
import math

import jax
import jax.numpy as jnp
from jax import lax
from jax.experimental import pallas as pl
from jax.experimental.pallas import tpu as pltpu
from jax.sharding import PartitionSpec as P

HD = 128
MESH = pl.DeviceIdType.MESH
F32 = jnp.float32
BF16 = jnp.bfloat16
NT = (((1,), (1,)), ((), ()))
DIRS = (1, -1)


class Tree:
    def __init__(self, half, step):
        self.half = half
        self.relays = tuple(range(0, half, step))

    def up(self, d):
        return max(r for r in self.relays if r < d)

    def below(self, r, sign):
        if r not in self.relays:
            return []
        return [d for d in range(self.far(sign), 0, -1) if self.up(d) == r]

    def far(self, sign):
        return self.half if sign == 1 else self.half - 1

    def hops(self):
        return {d - self.up(d) for d in range(1, self.half + 1)}


def split(x):
    high = x.astype(BF16).astype(F32)
    rest = x - high
    middle = rest.astype(BF16).astype(F32)
    return high, middle, rest - middle


def kernel(
    cfg,
    text_hbm, q_hbm, o_hbm, k_hbm, v_hbm, gate_ref,
    out_ref,
    text_v, q_v, o_v, k_v, v_v, vt_v, load_sem,
    part, ps_out, ps_in, ps_send, ps_recv,
    q_own, q_in, q_send, q_recv,
    acc_loc, stat_loc, st_out, st_in, st_send, st_recv,
    at_own, at_in, at_send, at_recv,
    own_x, x_out, x_in, x_send, x_recv,
    fin, f_send, f_recv,
):
    n, m, half, trees, block, unroll = cfg
    tree_p, tree_q, tree_s, tree_a = trees
    z = lax.axis_index("tok")
    x = lax.axis_index("head")
    rows = text_hbm.shape[0]
    depth = text_hbm.shape[1]
    piece = rows // n
    wide = q_hbm.shape[1]
    heads = wide // HD
    nq = heads * piece
    tokens = k_hbm.shape[0]
    scale_in = 1.0 / (depth * n)

    loads = [
        pltpu.make_async_copy(src, dst, load_sem.at[i])
        for i, (src, dst) in enumerate(
            ((text_hbm, text_v), (q_hbm, q_v), (v_hbm, v_v), (k_hbm, k_v), (o_hbm, o_v))
        )
    ]
    for c in loads:
        c.start()

    reach = sorted({(s * h) % n for t in trees for h in t.hops() for s in DIRS} - {0})
    barrier = pltpu.get_barrier_semaphore()
    for h in reach:
        pl.semaphore_signal(
            barrier, inc=1, device_id={"tok": lax.rem(z + h, n)}, device_id_type=MESH
        )
    for j in range(1, m):
        pl.semaphore_signal(
            barrier, inc=1, device_id={"head": lax.rem(x + j, m)}, device_id_type=MESH
        )

    def at(sign, d):
        return lax.rem(z + sign * d + 2 * n, n)

    def rows_of(p):
        return pl.ds(pl.multiple_of(p * piece, piece), piece)

    def along_z(src, dst, send, recv, sign, hop):
        return pltpu.make_async_remote_copy(
            src_ref=src, dst_ref=dst, send_sem=send, recv_sem=recv,
            device_id={"tok": at(sign, hop)}, device_id_type=MESH,
        )

    def lane(i):
        return pl.ds(i * nq, nq)

    loads[0].wait()
    loads[1].wait()
    text = text_v[...]
    hidden = text.astype(F32)
    first = lax.broadcasted_iota(jnp.int32, (rows, HD), 1) == 0
    squares = jnp.sum(hidden * hidden, axis=1, keepdims=True)
    part[:, wide:] = jnp.where(first, jnp.broadcast_to(squares, (rows, HD)), 0.0)
    cut = 256 if wide % 256 == 0 else 128
    for c in range(wide // cut):
        part[:, c * cut : (c + 1) * cut] = jnp.dot(
            text, q_v[:, c * cut : (c + 1) * cut], preferred_element_type=F32
        )

    def ps_copy(i, d):
        sign = DIRS[i]
        return along_z(
            ps_out.at[i, d], ps_in.at[i, d], ps_send.at[i, d], ps_recv.at[i, d],
            sign, d - tree_p.up(d),
        )

    lanes = lax.broadcasted_iota(jnp.int32, (piece, HD), 1)

    def gather_part(i_list, r, owner):
        main = part[rows_of(owner), :wide]
        tail = part[rows_of(owner), wide:]
        for i in i_list:
            for d in tree_p.below(r, DIRS[i]):
                ps_copy(i, d).wait_recv()
                main = main + ps_in[i, d, :, :wide].astype(F32)
                tail = tail + ps_in[i, d, :, wide:].astype(F32)
        return main, jnp.sum(tail, axis=1, keepdims=True)

    def send_part(i, d):
        main, sums = gather_part([i], d, at(DIRS[i], d))
        high = sums.astype(BF16).astype(F32)
        low = sums - high
        ps_out[i, d, :, :wide] = main.astype(BF16)
        ps_out[i, d, :, wide:] = jnp.where(
            lanes == 0, high, jnp.where(lanes == 1, low, 0.0)
        ).astype(BF16)
        ps_copy(i, d).start()

    pl.semaphore_wait(barrier, len(reach) + m - 1)

    todo = [(d, i) for d in range(half, 0, -1) for i in (0, 1) if d <= tree_p.far(DIRS[i])]
    leaves = [(d, i) for d, i in todo if not tree_p.below(d, DIRS[i])]
    inner = [(d, i) for d, i in todo if tree_p.below(d, DIRS[i])]
    for d, i in leaves:
        send_part(i, d)

    loads[2].wait()
    for c in range(0, tokens, block):
        vt_v[:, c : c + block] = v_v[c : c + block, :].astype(F32).T.astype(BF16)

    for d, i in inner:
        send_part(i, d)

    main, sums = gather_part([0, 1], 0, z)
    norm = lax.rsqrt(sums * scale_in + 1e-05) * (math.log2(math.e) / math.sqrt(HD))
    queries = (main * norm).astype(BF16)
    for g in range(heads):
        q_own[g * piece : (g + 1) * piece, :] = queries[:, g * HD : (g + 1) * HD]

    def q_copy(i, d):
        up = tree_q.up(d)
        src = q_own if up == 0 else q_in.at[up, lane(i)]
        return along_z(
            src, q_in.at[d, lane(i)], q_send.at[i, d], q_recv.at[i, d], DIRS[i], d - up
        )

    def forward_q(r):
        for i in (0, 1):
            if r:
                if r > tree_q.far(DIRS[i]):
                    continue
                q_copy(i, r).wait_recv()
            for d in tree_q.below(r, DIRS[i]):
                q_copy(i, d).start()

    forward_q(0)
    loads[3].wait()

    def attend(q):
        width = q.shape[0]

        def step(b, state):
            running, total, accum = state
            for u in range(unroll):
                start = pl.multiple_of((b * unroll + u) * block, block)
                scores = lax.dot_general(
                    k_v[pl.ds(start, block), :], q, NT, preferred_element_type=F32
                )
                newmax = jnp.maximum(running, jnp.max(scores, axis=0, keepdims=True))
                weights = jnp.exp2(scores - newmax)
                factor = jnp.exp2(running - newmax)
                total = total * factor + jnp.sum(weights, axis=0, keepdims=True)
                accum = accum * factor + jnp.dot(
                    vt_v[:, pl.ds(start, block)], weights.astype(BF16),
                    preferred_element_type=F32,
                )
                running = newmax
            return running, total, accum

        start = (
            jnp.full((1, width), -1e30, F32),
            jnp.zeros((1, width), F32),
            jnp.zeros((HD, width), F32),
        )
        return lax.fori_loop(0, tokens // (block * unroll), step, start)

    def st_copy(i, e):
        return along_z(
            st_out.at[i, e], st_in.at[i, e], st_send.at[i, e], st_recv.at[i, e],
            DIRS[i], e - tree_s.up(e),
        )

    stat_row = lax.broadcasted_iota(jnp.int32, (16, nq), 0)

    def send_state(i, e, running, total, accum):
        st_out[i, e, :HD, :] = accum.astype(BF16)
        stats = jnp.zeros((16, nq), F32)
        for k, term in enumerate(split(running) + split(total)):
            stats = jnp.where(stat_row == k, term, stats)
        st_out[i, e, HD:, :] = stats.astype(BF16)
        st_copy(i, e).start()

    def merged(i_list, e, d, i_own):
        running = stat_loc[i_own, d, 0:1, :]
        total = stat_loc[i_own, d, 1:2, :]
        accum = acc_loc[i_own, d]
        for i in i_list:
            for c in tree_s.below(e, DIRS[i]):
                st_copy(i, c).wait_recv()
                stats = st_in[i, c, HD:, :].astype(F32)
                peer_max = stats[0:1] + stats[1:2] + stats[2:3]
                peer_total = stats[3:4] + stats[4:5] + stats[5:6]
                newmax = jnp.maximum(running, peer_max)
                mine, theirs = jnp.exp2(running - newmax), jnp.exp2(peer_max - newmax)
                total = total * mine + peer_total * theirs
                accum = accum * mine + st_in[i, c, :HD, :].astype(F32) * theirs
                running = newmax
        return running, total, accum

    def finish_state(d):
        e = half - d
        for i in (0, 1):
            if 1 <= e <= tree_s.far(DIRS[i]) and tree_s.below(e, DIRS[i]):
                send_state(i, e, *merged([i], e, d, i))

    def attend_piece(d):
        both = 0 < d < half
        q = q_own[...] if d == 0 else (q_in[d] if both else q_in[d, 0:nq, :])
        running, total, accum = attend(q)
        e = half - d
        for i in (0, 1) if both else (0,):
            cols = slice(i * nq, (i + 1) * nq)
            r, t, a = running[:, cols], total[:, cols], accum[:, cols]
            if e and not tree_s.below(e, DIRS[i]):
                send_state(i, e, r, t, a)
            else:
                stat_loc[i, d, 0:1, :] = r
                stat_loc[i, d, 1:2, :] = t
                acc_loc[i, d] = a

    late = []
    forwarded = {0}
    for d in range(half + 1):
        for r in (d, d + 1):
            if r in tree_q.relays and r not in forwarded:
                forward_q(r)
                forwarded.add(r)
        if d and d not in forwarded:
            for i in (0, 1):
                if d <= tree_q.far(DIRS[i]):
                    q_copy(i, d).wait_recv()
        attend_piece(d)
        while late:
            finish_state(late.pop())
        late.append(d)

    _, total, accum = merged([0, 1], 0, half, 0)
    attended = (accum / total).T
    for g in range(heads):
        at_own[:, g * HD : (g + 1) * HD] = attended[g * piece : (g + 1) * piece, :].astype(BF16)

    def at_copy(i, d):
        up = tree_a.up(d)
        span = pl.ds(i * piece, piece)
        src = at_own if up == 0 else at_in.at[up, span]
        return along_z(
            src, at_in.at[d, span], at_send.at[i, d], at_recv.at[i, d], DIRS[i], d - up
        )

    def forward_a(r):
        for i in (0, 1):
            if r:
                if r > tree_a.far(DIRS[i]):
                    continue
                at_copy(i, r).wait_recv()
            for d in tree_a.below(r, DIRS[i]):
                at_copy(i, d).start()

    def place(i, d):
        p = lax.rem(z - DIRS[i] * d + half + n, n)
        which = lax.div(p, m)
        owner = lax.rem(p, m)
        return which, owner, lax.rem(x - owner + m, m)

    def x_copy(i, d):
        which, owner, j = place(i, d)
        return pltpu.make_async_remote_copy(
            src_ref=x_out.at[i, d], dst_ref=x_in.at[which, j],
            send_sem=x_send.at[i, d], recv_sem=x_recv.at[which, j],
            device_id={"head": owner}, device_id_type=MESH,
        )

    def project(d):
        both = 0 < d < half
        a = at_own[...] if d == 0 else (at_in[d] if both else at_in[d, 0:piece, :])
        branch = jnp.dot(a, o_v[...], preferred_element_type=F32)
        for i in (0, 1) if both else (0,):
            term = branch[i * piece : (i + 1) * piece, :]
            which, owner, j = place(i, d)

            @pl.when(j == 0)
            def _():
                own_x[which] = term

            @pl.when(j != 0)
            def _():
                x_out[i, d] = term.astype(BF16)
                x_copy(i, d).start()

    def f_copy(which, j):
        p = x + which * m
        return pltpu.make_async_remote_copy(
            src_ref=fin.at[which], dst_ref=out_ref.at[rows_of(p)],
            send_sem=f_send.at[which, j], recv_sem=f_recv.at[which, j],
            device_id={"head": lax.rem(x + j, m)}, device_id_type=MESH,
        )

    strength = jnp.tanh(jnp.full((piece, depth), gate_ref[0], F32))

    def finish_rows(which):
        branch = own_x[which]
        for j in range(1, m):
            pltpu.make_async_remote_copy(
                src_ref=fin.at[0], dst_ref=x_in.at[which, j],
                send_sem=f_send.at[0, 0], recv_sem=x_recv.at[which, j],
                device_id={"head": lax.rem(x + j, m)}, device_id_type=MESH,
            ).wait_recv()
            branch = branch + x_in[which, j].astype(F32)
        p = x + which * m
        done = (text_v[rows_of(p), :].astype(F32) + strength * branch).astype(BF16)
        fin[which] = done
        for j in range(1, m):
            f_copy(which, j).start()
        out_ref[rows_of(p), :] = done

    loads[4].wait()
    forward_a(0)
    forwarded = {0}
    early = lax.div(lax.rem(z + half - x + n + half // 2, n), half + 1)
    for d in range(half + 1):
        for r in (d, d + 1):
            if r in tree_a.relays and r not in forwarded:
                forward_a(r)
                forwarded.add(r)
        if d and d not in forwarded:
            for i in (0, 1):
                if d <= tree_a.far(DIRS[i]):
                    at_copy(i, d).wait_recv()
        project(d)
        if d == half - 1:
            finish_rows(early)
    finish_rows(1 - early)

    for j in range(1, m):
        for which in (0, 1):
            p = lax.rem(x - j + m, m) + which * m
            pltpu.make_async_remote_copy(
                src_ref=fin.at[which], dst_ref=out_ref.at[rows_of(p)],
                send_sem=f_send.at[which, j], recv_sem=f_recv.at[which, j],
                device_id={"head": lax.rem(x + j, m)}, device_id_type=MESH,
            ).wait_recv()

    for i in (0, 1):
        for d in range(1, tree_p.far(DIRS[i]) + 1):
            ps_copy(i, d).wait_send()
            q_copy(i, d).wait_send()
            st_copy(i, d).wait_send()
            at_copy(i, d).wait_send()
        for d in range(0, half + 1):
            if i == 1 and d in (0, half):
                continue
            _, _, j = place(i, d)

            @pl.when(j != 0)
            def _():
                x_copy(i, d).wait_send()

    for which in (0, 1):
        for j in range(1, m):
            f_copy(which, j).wait_send()


STEPS = (2, 2, 2, 2)
BLOCK = 512
UNROLL = 4


def body(text, q_weight, out_weight, keys, values, gate):
    n, m = lax.axis_size("tok"), lax.axis_size("head")
    half = n // 2
    assert n == 2 * m and keys.shape[1] == HD
    rows, depth = text.shape
    wide = q_weight.shape[1]
    tokens = keys.shape[0]
    piece = rows // n
    heads = wide // HD
    nq = heads * piece
    block = min(BLOCK, tokens)
    unroll = min(UNROLL, tokens // block)
    trees = tuple(Tree(half, s) for s in STEPS)
    vm, dma = pltpu.VMEM, pltpu.SemaphoreType.DMA
    slots = (2, half + 1)
    scratch = [
        vm((rows, depth), BF16), vm((depth, wide), BF16), vm((wide, depth), BF16),
        vm((tokens, HD), BF16), vm((tokens, HD), BF16), vm((HD, tokens), BF16), dma((5,)),
        vm((rows, wide + HD), F32),
        vm((*slots, piece, wide + HD), BF16), vm((*slots, piece, wide + HD), BF16), dma(slots), dma(slots),
        vm((nq, HD), BF16), vm((half + 1, 2 * nq, HD), BF16), dma(slots), dma(slots),
        vm((*slots, HD, nq), F32), vm((*slots, 8, nq), F32),
        vm((*slots, HD + 16, nq), BF16), vm((*slots, HD + 16, nq), BF16), dma(slots), dma(slots),
        vm((piece, wide), BF16), vm((half + 1, 2 * piece, wide), BF16), dma(slots), dma(slots),
        vm((2, piece, depth), F32), vm((*slots, piece, depth), BF16), vm((2, m, piece, depth), BF16),
        dma(slots), dma((2, m)),
        vm((2, piece, depth), BF16), dma((2, m)), dma((2, m)),
    ]
    hbm = pl.BlockSpec(memory_space=pl.ANY)
    return pl.pallas_call(
        functools.partial(kernel, (n, m, half, trees, block, unroll)),
        out_shape=jax.ShapeDtypeStruct((rows, depth), BF16),
        in_specs=[hbm] * 5 + [pl.BlockSpec(memory_space=pltpu.SMEM)],
        out_specs=pl.BlockSpec(memory_space=pltpu.VMEM),
        scratch_shapes=scratch,
        compiler_params=pltpu.CompilerParams(
            collective_id=0, has_side_effects=True, vmem_limit_bytes=48 * 1024 * 1024
        ),
    )(text, q_weight, out_weight, keys, values, gate)


def solution(mesh):
    in_specs = (
        P(("groups", "row"), "tok"),
        P("tok", "head"),
        P("head", "tok"),
        P(("groups", "tok"), "head"),
        P(("groups", "tok"), "head"),
        P(),
    )
    out_specs = P(("groups", "row"), "tok")
    return jax.shard_map(body, mesh=mesh, in_specs=in_specs, out_specs=out_specs, check_vma=False)
```

```python
import functools
import math

import jax
import jax.numpy as jnp
from jax import lax
from jax.experimental import pallas as pl
from jax.experimental.pallas import tpu as pltpu
from jax.sharding import PartitionSpec as P

HD = 128
MESH = pl.DeviceIdType.MESH
F32 = jnp.float32
BF16 = jnp.bfloat16
NT = (((1,), (1,)), ((), ()))
DIRS = (1, -1)


class Tree:
    def __init__(self, half, step):
        self.half = half
        self.relays = tuple(range(0, half, step))

    def up(self, d):
        return max(r for r in self.relays if r < d)

    def below(self, r, sign):
        if r not in self.relays:
            return []
        return [d for d in range(self.far(sign), 0, -1) if self.up(d) == r]

    def far(self, sign):
        return self.half if sign == 1 else self.half - 1

    def hops(self):
        return {d - self.up(d) for d in range(1, self.half + 1)}


def split(x):
    high = x.astype(BF16).astype(F32)
    rest = x - high
    middle = rest.astype(BF16).astype(F32)
    return high, middle, rest - middle


def kernel(
    cfg,
    text_hbm, q_hbm, o_hbm, k_hbm, v_hbm, gate_ref,
    out_ref,
    text_v, q_v, o_v, k_v, v_v, vt_v, load_sem, scores_v,
    part, ps_out, ps_in, ps_send, ps_recv,
    q_own, q_in, q_send, q_recv,
    acc_loc, stat_loc, st_out, st_in, st_send, st_recv,
    at_own, at_in, at_send, at_recv,
    own_x, x_out, x_in, x_send, x_recv,
    fin, f_send, f_recv,
):
    n, m, half, trees, block = cfg
    tree_p, tree_q, tree_s, tree_a = trees
    z = lax.axis_index("tok")
    x = lax.axis_index("head")
    rows = text_hbm.shape[0]
    depth = text_hbm.shape[1]
    piece = rows // n
    wide = q_hbm.shape[1]
    heads = wide // HD
    nq = heads * piece
    tokens = k_hbm.shape[0]
    scale_in = 1.0 / (depth * n)

    loads = [
        pltpu.make_async_copy(src, dst, load_sem.at[i])
        for i, (src, dst) in enumerate(
            ((text_hbm, text_v), (q_hbm, q_v), (v_hbm, v_v), (k_hbm, k_v), (o_hbm, o_v))
        )
    ]
    loads[0].start()
    loads[1].start()

    reach = sorted({(s * h) % n for t in trees for h in t.hops() for s in DIRS} - {0})
    barrier = pltpu.get_barrier_semaphore()
    for h in reach:
        pl.semaphore_signal(
            barrier, inc=1, device_id={"tok": lax.rem(z + h, n)}, device_id_type=MESH
        )
    for j in range(1, m):
        pl.semaphore_signal(
            barrier, inc=1, device_id={"head": lax.rem(x + j, m)}, device_id_type=MESH
        )

    def at(sign, d):
        return lax.rem(z + sign * d + 2 * n, n)

    def rows_of(p):
        return pl.ds(pl.multiple_of(p * piece, piece), piece)

    def along_z(src, dst, send, recv, sign, hop):
        return pltpu.make_async_remote_copy(
            src_ref=src, dst_ref=dst, send_sem=send, recv_sem=recv,
            device_id={"tok": at(sign, hop)}, device_id_type=MESH,
        )

    def lane(i):
        return pl.ds(i * nq, nq)

    loads[0].wait()
    loads[1].wait()
    for c in loads[2:]:
        c.start()
    text = text_v[...]
    hidden = text.astype(F32)
    first = lax.broadcasted_iota(jnp.int32, (rows, HD), 1) == 0
    squares = jnp.sum(hidden * hidden, axis=1, keepdims=True)
    part[:, wide:] = jnp.where(first, jnp.broadcast_to(squares, (rows, HD)), 0.0)
    cut = 256 if wide % 256 == 0 else 128
    for c in range(wide // cut):
        part[:, c * cut : (c + 1) * cut] = jnp.dot(
            text, q_v[:, c * cut : (c + 1) * cut], preferred_element_type=F32
        )

    def ps_copy(i, d):
        sign = DIRS[i]
        return along_z(
            ps_out.at[i, d], ps_in.at[i, d], ps_send.at[i, d], ps_recv.at[i, d],
            sign, d - tree_p.up(d),
        )

    lanes = lax.broadcasted_iota(jnp.int32, (piece, HD), 1)

    def gather_part(i_list, r, owner):
        main = part[rows_of(owner), :wide]
        tail = part[rows_of(owner), wide:]
        for i in i_list:
            for d in tree_p.below(r, DIRS[i]):
                ps_copy(i, d).wait_recv()
                main = main + ps_in[i, d, :, :wide].astype(F32)
                tail = tail + ps_in[i, d, :, wide:].astype(F32)
        return main, jnp.sum(tail, axis=1, keepdims=True)

    def send_part(i, d):
        main, sums = gather_part([i], d, at(DIRS[i], d))
        high = sums.astype(BF16).astype(F32)
        low = sums - high
        ps_out[i, d, :, :wide] = main.astype(BF16)
        ps_out[i, d, :, wide:] = jnp.where(
            lanes == 0, high, jnp.where(lanes == 1, low, 0.0)
        ).astype(BF16)
        ps_copy(i, d).start()

    pl.semaphore_wait(barrier, len(reach) + m - 1)

    todo = [(d, i) for d in range(half, 0, -1) for i in (0, 1) if d <= tree_p.far(DIRS[i])]
    leaves = [(d, i) for d, i in todo if not tree_p.below(d, DIRS[i])]
    inner = [(d, i) for d, i in todo if tree_p.below(d, DIRS[i])]
    for d, i in leaves:
        send_part(i, d)

    for d, i in inner:
        send_part(i, d)

    main, sums = gather_part([0, 1], 0, z)
    norm = lax.rsqrt(sums * scale_in + 1e-05) * (math.log2(math.e) / math.sqrt(HD))
    queries = (main * norm).astype(BF16)
    for g in range(heads):
        q_own[g * piece : (g + 1) * piece, :] = queries[:, g * HD : (g + 1) * HD]

    def q_copy(i, d):
        up = tree_q.up(d)
        src = q_own if up == 0 else q_in.at[up, lane(i)]
        return along_z(
            src, q_in.at[d, lane(i)], q_send.at[i, d], q_recv.at[i, d], DIRS[i], d - up
        )

    def forward_q(r):
        for i in (0, 1):
            if r:
                if r > tree_q.far(DIRS[i]):
                    continue
                q_copy(i, r).wait_recv()
            for d in tree_q.below(r, DIRS[i]):
                q_copy(i, d).start()

    forward_q(0)
    loads[2].wait()
    for c in range(0, tokens, block):
        vt_v[:, c : c + block] = v_v[c : c + block, :].astype(F32).T.astype(BF16)
    loads[3].wait()

    def attend(q):
        width = q.shape[0]
        cols = slice(0, width)
        top = jnp.full((8, width), -1e30, F32)
        for b in range(0, tokens, block):
            scores = lax.dot_general(k_v[b : b + block, :], q, NT, preferred_element_type=F32)
            scores_v[b : b + block, cols] = scores
            top = jnp.maximum(top, jnp.max(scores.reshape(block // 8, 8, width), axis=0))
        running = jnp.max(top, axis=0, keepdims=True)
        sums = jnp.zeros((8, width), F32)
        accum = jnp.zeros((HD, width), F32)
        for b in range(0, tokens, block):
            weights = jnp.exp2(scores_v[b : b + block, cols] - running)
            sums = sums + jnp.sum(weights.reshape(block // 8, 8, width), axis=0)
            accum = accum + jnp.dot(
                vt_v[:, b : b + block], weights.astype(BF16), preferred_element_type=F32
            )
        return running, jnp.sum(sums, axis=0, keepdims=True), accum

    def st_copy(i, e):
        return along_z(
            st_out.at[i, e], st_in.at[i, e], st_send.at[i, e], st_recv.at[i, e],
            DIRS[i], e - tree_s.up(e),
        )

    stat_row = lax.broadcasted_iota(jnp.int32, (16, nq), 0)

    def send_state(i, e, running, total, accum):
        st_out[i, e, :HD, :] = accum.astype(BF16)
        stats = jnp.zeros((16, nq), F32)
        for k, term in enumerate(split(running) + split(total)):
            stats = jnp.where(stat_row == k, term, stats)
        st_out[i, e, HD:, :] = stats.astype(BF16)
        st_copy(i, e).start()

    def merged(i_list, e, d, i_own):
        running = stat_loc[i_own, d, 0:1, :]
        total = stat_loc[i_own, d, 1:2, :]
        accum = acc_loc[i_own, d]
        for i in i_list:
            for c in tree_s.below(e, DIRS[i]):
                st_copy(i, c).wait_recv()
                stats = st_in[i, c, HD:, :].astype(F32)
                peer_max = stats[0:1] + stats[1:2] + stats[2:3]
                peer_total = stats[3:4] + stats[4:5] + stats[5:6]
                newmax = jnp.maximum(running, peer_max)
                mine, theirs = jnp.exp2(running - newmax), jnp.exp2(peer_max - newmax)
                total = total * mine + peer_total * theirs
                accum = accum * mine + st_in[i, c, :HD, :].astype(F32) * theirs
                running = newmax
        return running, total, accum

    def finish_state(d):
        e = half - d
        for i in (0, 1):
            if 1 <= e <= tree_s.far(DIRS[i]) and tree_s.below(e, DIRS[i]):
                send_state(i, e, *merged([i], e, d, i))

    def attend_piece(d):
        both = 0 < d < half
        q = q_own[...] if d == 0 else (q_in[d] if both else q_in[d, 0:nq, :])
        running, total, accum = attend(q)
        e = half - d
        for i in (0, 1) if both else (0,):
            cols = slice(i * nq, (i + 1) * nq)
            r, t, a = running[:, cols], total[:, cols], accum[:, cols]
            if e and not tree_s.below(e, DIRS[i]):
                send_state(i, e, r, t, a)
            else:
                stat_loc[i, d, 0:1, :] = r
                stat_loc[i, d, 1:2, :] = t
                acc_loc[i, d] = a

    late = []
    forwarded = {0}
    for d in range(half + 1):
        for r in (d, d + 1):
            if r in tree_q.relays and r not in forwarded:
                forward_q(r)
                forwarded.add(r)
        if d and d not in forwarded:
            for i in (0, 1):
                if d <= tree_q.far(DIRS[i]):
                    q_copy(i, d).wait_recv()
        attend_piece(d)
        while late:
            finish_state(late.pop())
        late.append(d)

    _, total, accum = merged([0, 1], 0, half, 0)
    attended = (accum / total).T
    for g in range(heads):
        at_own[:, g * HD : (g + 1) * HD] = attended[g * piece : (g + 1) * piece, :].astype(BF16)

    def at_copy(i, d):
        up = tree_a.up(d)
        span = pl.ds(i * piece, piece)
        src = at_own if up == 0 else at_in.at[up, span]
        return along_z(
            src, at_in.at[d, span], at_send.at[i, d], at_recv.at[i, d], DIRS[i], d - up
        )

    def forward_a(r):
        for i in (0, 1):
            if r:
                if r > tree_a.far(DIRS[i]):
                    continue
                at_copy(i, r).wait_recv()
            for d in tree_a.below(r, DIRS[i]):
                at_copy(i, d).start()

    def place(i, d):
        p = lax.rem(z - DIRS[i] * d + half + n, n)
        which = lax.div(p, m)
        owner = lax.rem(p, m)
        return which, owner, lax.rem(x - owner + m, m)

    def x_copy(i, d):
        which, owner, j = place(i, d)
        return pltpu.make_async_remote_copy(
            src_ref=x_out.at[i, d], dst_ref=x_in.at[which, j],
            send_sem=x_send.at[i, d], recv_sem=x_recv.at[which, j],
            device_id={"head": owner}, device_id_type=MESH,
        )

    def project(d):
        both = 0 < d < half
        a = at_own[...] if d == 0 else (at_in[d] if both else at_in[d, 0:piece, :])
        branch = jnp.dot(a, o_v[...], preferred_element_type=F32)
        for i in (0, 1) if both else (0,):
            term = branch[i * piece : (i + 1) * piece, :]
            which, owner, j = place(i, d)

            @pl.when(j == 0)
            def _():
                own_x[which] = term

            @pl.when(j != 0)
            def _():
                x_out[i, d] = term.astype(BF16)
                x_copy(i, d).start()

    def f_copy(which, j):
        p = x + which * m
        return pltpu.make_async_remote_copy(
            src_ref=fin.at[which], dst_ref=out_ref.at[rows_of(p)],
            send_sem=f_send.at[which, j], recv_sem=f_recv.at[which, j],
            device_id={"head": lax.rem(x + j, m)}, device_id_type=MESH,
        )

    strength = jnp.tanh(jnp.full((piece, depth), gate_ref[0], F32))

    def finish_rows(which):
        branch = own_x[which]
        for j in range(1, m):
            pltpu.make_async_remote_copy(
                src_ref=fin.at[0], dst_ref=x_in.at[which, j],
                send_sem=f_send.at[0, 0], recv_sem=x_recv.at[which, j],
                device_id={"head": lax.rem(x + j, m)}, device_id_type=MESH,
            ).wait_recv()
            branch = branch + x_in[which, j].astype(F32)
        p = x + which * m
        done = (text_v[rows_of(p), :].astype(F32) + strength * branch).astype(BF16)
        fin[which] = done
        for j in sorted(range(1, m), key=lambda j: -min(j, m - j)):
            f_copy(which, j).start()
        out_ref[rows_of(p), :] = done

    loads[4].wait()
    forward_a(0)
    forwarded = {0}
    early = lax.div(lax.rem(z + half - x + n + half // 2, n), half + 1)
    for d in range(half + 1):
        for r in (d, d + 1):
            if r in tree_a.relays and r not in forwarded:
                forward_a(r)
                forwarded.add(r)
        if d and d not in forwarded:
            for i in (0, 1):
                if d <= tree_a.far(DIRS[i]):
                    at_copy(i, d).wait_recv()
        project(d)
        if d == max(half // 2, half - 2):
            finish_rows(early)
    finish_rows(1 - early)

    for j in range(1, m):
        for which in (0, 1):
            p = lax.rem(x - j + m, m) + which * m
            pltpu.make_async_remote_copy(
                src_ref=fin.at[which], dst_ref=out_ref.at[rows_of(p)],
                send_sem=f_send.at[which, j], recv_sem=f_recv.at[which, j],
                device_id={"head": lax.rem(x + j, m)}, device_id_type=MESH,
            ).wait_recv()

    for i in (0, 1):
        for d in range(1, tree_p.far(DIRS[i]) + 1):
            ps_copy(i, d).wait_send()
            q_copy(i, d).wait_send()
            st_copy(i, d).wait_send()
            at_copy(i, d).wait_send()
        for d in range(0, half + 1):
            if i == 1 and d in (0, half):
                continue
            _, _, j = place(i, d)

            @pl.when(j != 0)
            def _():
                x_copy(i, d).wait_send()

    for which in (0, 1):
        for j in range(1, m):
            f_copy(which, j).wait_send()


STEPS = (2, 2, 2, 2)
BLOCK = 256


def body(text, q_weight, out_weight, keys, values, gate):
    n, m = lax.axis_size("tok"), lax.axis_size("head")
    half = n // 2
    assert n == 2 * m and keys.shape[1] == HD
    rows, depth = text.shape
    wide = q_weight.shape[1]
    tokens = keys.shape[0]
    piece = rows // n
    heads = wide // HD
    nq = heads * piece
    block = min(BLOCK, tokens)
    trees = tuple(Tree(half, s) for s in STEPS)
    vm, dma = pltpu.VMEM, pltpu.SemaphoreType.DMA
    slots = (2, half + 1)
    scratch = [
        vm((rows, depth), BF16), vm((depth, wide), BF16), vm((wide, depth), BF16),
        vm((tokens, HD), BF16), vm((tokens, HD), BF16), vm((HD, tokens), BF16), dma((5,)),
        vm((tokens, 2 * nq), F32),
        vm((rows, wide + HD), F32),
        vm((*slots, piece, wide + HD), BF16), vm((*slots, piece, wide + HD), BF16), dma(slots), dma(slots),
        vm((nq, HD), BF16), vm((half + 1, 2 * nq, HD), BF16), dma(slots), dma(slots),
        vm((*slots, HD, nq), F32), vm((*slots, 8, nq), F32),
        vm((*slots, HD + 16, nq), BF16), vm((*slots, HD + 16, nq), BF16), dma(slots), dma(slots),
        vm((piece, wide), BF16), vm((half + 1, 2 * piece, wide), BF16), dma(slots), dma(slots),
        vm((2, piece, depth), F32), vm((*slots, piece, depth), BF16), vm((2, m, piece, depth), BF16),
        dma(slots), dma((2, m)),
        vm((2, piece, depth), BF16), dma((2, m)), dma((2, m)),
    ]
    hbm = pl.BlockSpec(memory_space=pl.ANY)
    return pl.pallas_call(
        functools.partial(kernel, (n, m, half, trees, block)),
        out_shape=jax.ShapeDtypeStruct((rows, depth), BF16),
        in_specs=[hbm] * 5 + [pl.BlockSpec(memory_space=pltpu.SMEM)],
        out_specs=pl.BlockSpec(memory_space=pltpu.VMEM),
        scratch_shapes=scratch,
        compiler_params=pltpu.CompilerParams(
            collective_id=0, has_side_effects=True, vmem_limit_bytes=67043328
        ),
    )(text, q_weight, out_weight, keys, values, gate)


def solution(mesh):
    in_specs = (
        P(("groups", "row"), "tok"),
        P("tok", "head"),
        P("head", "tok"),
        P(("groups", "tok"), "head"),
        P(("groups", "tok"), "head"),
        P(),
    )
    out_specs = P(("groups", "row"), "tok")
    return jax.shard_map(body, mesh=mesh, in_specs=in_specs, out_specs=out_specs, check_vma=False)
```

```python
import functools
import math

import jax
import jax.numpy as jnp
from jax import lax
from jax.experimental import pallas as pl
from jax.experimental.pallas import tpu as pltpu
from jax.sharding import PartitionSpec as P

HD = 128
MESH = pl.DeviceIdType.MESH
F32 = jnp.float32
BF16 = jnp.bfloat16
NT = (((1,), (1,)), ((), ()))
DIRS = (1, -1)


class Tree:
    def __init__(self, half, step):
        self.half = half
        self.relays = tuple(range(0, half, step))

    def up(self, d):
        return max(r for r in self.relays if r < d)

    def below(self, r, sign):
        if r not in self.relays:
            return []
        return [d for d in range(self.far(sign), 0, -1) if self.up(d) == r]

    def far(self, sign):
        return self.half if sign == 1 else self.half - 1

    def hops(self):
        return {d - self.up(d) for d in range(1, self.half + 1)}


def split(x):
    high = x.astype(BF16).astype(F32)
    rest = x - high
    middle = rest.astype(BF16).astype(F32)
    return high, middle, rest - middle


def kernel(
    cfg,
    text_hbm, q_hbm, o_hbm, k_hbm, v_hbm, gate_ref,
    out_ref,
    text_v, q_v, o_v, k_v, v_v, vt_v, load_sem, scores_v,
    part, ps_out, ps_in, ps_send, ps_recv,
    q_own, q_in, q_send, q_recv,
    acc_loc, stat_loc, st_out, st_in, st_send, st_recv,
    at_own, at_in, at_send, at_recv,
    own_x, x_out, x_in, x_send, x_recv,
    fin, f_send, f_recv,
):
    n, m, half, trees, block = cfg
    tree_p, tree_q, tree_s, tree_a = trees
    z = lax.axis_index("tok")
    x = lax.axis_index("head")
    rows = text_hbm.shape[0]
    depth = text_hbm.shape[1]
    piece = rows // n
    wide = q_hbm.shape[1]
    heads = wide // HD
    nq = heads * piece
    tokens = k_hbm.shape[0]
    scale_in = 1.0 / (depth * n)

    loads = [
        pltpu.make_async_copy(src, dst, load_sem.at[i])
        for i, (src, dst) in enumerate(
            ((text_hbm, text_v), (q_hbm, q_v), (v_hbm, v_v), (k_hbm, k_v), (o_hbm, o_v))
        )
    ]
    loads[0].start()
    loads[1].start()

    reach = sorted({(s * h) % n for t in trees for h in t.hops() for s in DIRS} - {0})
    barrier = pltpu.get_barrier_semaphore()
    for h in reach:
        pl.semaphore_signal(
            barrier, inc=1, device_id={"tok": lax.rem(z + h, n)}, device_id_type=MESH
        )
    for j in range(1, m):
        pl.semaphore_signal(
            barrier, inc=1, device_id={"head": lax.rem(x + j, m)}, device_id_type=MESH
        )

    def at(sign, d):
        return lax.rem(z + sign * d + 2 * n, n)

    def rows_of(p):
        return pl.ds(pl.multiple_of(p * piece, piece), piece)

    def along_z(src, dst, send, recv, sign, hop):
        return pltpu.make_async_remote_copy(
            src_ref=src, dst_ref=dst, send_sem=send, recv_sem=recv,
            device_id={"tok": at(sign, hop)}, device_id_type=MESH,
        )

    def lane(i):
        return pl.ds(i * nq, nq)

    loads[0].wait()
    loads[1].wait()
    for c in loads[2:]:
        c.start()
    text = text_v[...]
    hidden = text.astype(F32)
    first = lax.broadcasted_iota(jnp.int32, (rows, HD), 1) == 0
    squares = jnp.sum(hidden * hidden, axis=1, keepdims=True)
    part[:, wide:] = jnp.where(first, jnp.broadcast_to(squares, (rows, HD)), 0.0)
    cut = 256 if wide % 256 == 0 else 128
    for c in range(wide // cut):
        part[:, c * cut : (c + 1) * cut] = jnp.dot(
            text, q_v[:, c * cut : (c + 1) * cut], preferred_element_type=F32
        )

    def ps_copy(i, d):
        sign = DIRS[i]
        return along_z(
            ps_out.at[i, d], ps_in.at[i, d], ps_send.at[i, d], ps_recv.at[i, d],
            sign, d - tree_p.up(d),
        )

    lanes = lax.broadcasted_iota(jnp.int32, (piece, HD), 1)

    def gather_part(i_list, r, owner):
        main = part[rows_of(owner), :wide]
        tail = part[rows_of(owner), wide:]
        for i in i_list:
            for d in tree_p.below(r, DIRS[i]):
                ps_copy(i, d).wait_recv()
                main = main + ps_in[i, d, :, :wide].astype(F32)
                tail = tail + ps_in[i, d, :, wide:].astype(F32)
        return main, jnp.sum(tail, axis=1, keepdims=True)

    def send_part(i, d):
        main, sums = gather_part([i], d, at(DIRS[i], d))
        high = sums.astype(BF16).astype(F32)
        low = sums - high
        ps_out[i, d, :, :wide] = main.astype(BF16)
        ps_out[i, d, :, wide:] = jnp.where(
            lanes == 0, high, jnp.where(lanes == 1, low, 0.0)
        ).astype(BF16)
        ps_copy(i, d).start()

    pl.semaphore_wait(barrier, len(reach) + m - 1)

    todo = [(d, i) for d in range(half, 0, -1) for i in (0, 1) if d <= tree_p.far(DIRS[i])]
    leaves = [(d, i) for d, i in todo if not tree_p.below(d, DIRS[i])]
    inner = [(d, i) for d, i in todo if tree_p.below(d, DIRS[i])]
    for d, i in leaves:
        send_part(i, d)

    for d, i in inner:
        send_part(i, d)

    main, sums = gather_part([0, 1], 0, z)
    norm = lax.rsqrt(sums * scale_in + 1e-05) * (math.log2(math.e) / math.sqrt(HD))
    queries = (main * norm).astype(BF16)
    for g in range(heads):
        q_own[g * piece : (g + 1) * piece, :] = queries[:, g * HD : (g + 1) * HD]

    def q_copy(i, d):
        up = tree_q.up(d)
        src = q_own if up == 0 else q_in.at[up, lane(i)]
        return along_z(
            src, q_in.at[d, lane(i)], q_send.at[i, d], q_recv.at[i, d], DIRS[i], d - up
        )

    def forward_q(r):
        for i in (0, 1):
            if r:
                if r > tree_q.far(DIRS[i]):
                    continue
                q_copy(i, r).wait_recv()
            for d in tree_q.below(r, DIRS[i]):
                q_copy(i, d).start()

    forward_q(0)
    loads[2].wait()
    for c in range(0, tokens, block):
        vt_v[:, c : c + block] = v_v[c : c + block, :].astype(F32).T.astype(BF16)
    loads[3].wait()

    def attend(q):
        width = q.shape[0]
        cols = slice(0, width)
        top = jnp.full((8, width), -1e30, F32)
        for b in range(0, tokens, block):
            scores = lax.dot_general(k_v[b : b + block, :], q, NT, preferred_element_type=F32)
            scores_v[b : b + block, cols] = scores
            top = jnp.maximum(top, jnp.max(scores.reshape(block // 8, 8, width), axis=0))
        running = jnp.max(top, axis=0, keepdims=True)
        sums = jnp.zeros((8, width), F32)
        accum = jnp.zeros((HD, width), F32)
        for b in range(0, tokens, block):
            weights = jnp.exp2(scores_v[b : b + block, cols] - running)
            sums = sums + jnp.sum(weights.reshape(block // 8, 8, width), axis=0)
            accum = accum + jnp.dot(
                vt_v[:, b : b + block], weights.astype(BF16), preferred_element_type=F32
            )
        return running, jnp.sum(sums, axis=0, keepdims=True), accum

    def st_copy(i, e):
        return along_z(
            st_out.at[i, e], st_in.at[i, e], st_send.at[i, e], st_recv.at[i, e],
            DIRS[i], e - tree_s.up(e),
        )

    stat_row = lax.broadcasted_iota(jnp.int32, (16, nq), 0)

    def send_state(i, e, running, total, accum):
        st_out[i, e, :HD, :] = accum.astype(BF16)
        stats = jnp.zeros((16, nq), F32)
        for k, term in enumerate(split(running) + split(total)):
            stats = jnp.where(stat_row == k, term, stats)
        st_out[i, e, HD:, :] = stats.astype(BF16)
        st_copy(i, e).start()

    def merged(i_list, e, d, i_own):
        running = stat_loc[i_own, d, 0:1, :]
        total = stat_loc[i_own, d, 1:2, :]
        accum = acc_loc[i_own, d]
        for i in i_list:
            for c in tree_s.below(e, DIRS[i]):
                st_copy(i, c).wait_recv()
                stats = st_in[i, c, HD:, :].astype(F32)
                peer_max = stats[0:1] + stats[1:2] + stats[2:3]
                peer_total = stats[3:4] + stats[4:5] + stats[5:6]
                newmax = jnp.maximum(running, peer_max)
                mine, theirs = jnp.exp2(running - newmax), jnp.exp2(peer_max - newmax)
                total = total * mine + peer_total * theirs
                accum = accum * mine + st_in[i, c, :HD, :].astype(F32) * theirs
                running = newmax
        return running, total, accum

    def finish_state(d):
        e = half - d
        for i in (0, 1):
            if 1 <= e <= tree_s.far(DIRS[i]) and tree_s.below(e, DIRS[i]):
                send_state(i, e, *merged([i], e, d, i))

    def attend_piece(d):
        both = 0 < d < half
        q = q_own[...] if d == 0 else (q_in[d] if both else q_in[d, 0:nq, :])
        running, total, accum = attend(q)
        e = half - d
        for i in (0, 1) if both else (0,):
            cols = slice(i * nq, (i + 1) * nq)
            r, t, a = running[:, cols], total[:, cols], accum[:, cols]
            if e and not tree_s.below(e, DIRS[i]):
                send_state(i, e, r, t, a)
            else:
                stat_loc[i, d, 0:1, :] = r
                stat_loc[i, d, 1:2, :] = t
                acc_loc[i, d] = a

    late = []
    forwarded = {0}
    for d in range(half + 1):
        for r in (d, d + 1):
            if r in tree_q.relays and r not in forwarded:
                forward_q(r)
                forwarded.add(r)
        if d and d not in forwarded:
            for i in (0, 1):
                if d <= tree_q.far(DIRS[i]):
                    q_copy(i, d).wait_recv()
        attend_piece(d)
        while late:
            finish_state(late.pop())
        late.append(d)

    _, total, accum = merged([0, 1], 0, half, 0)
    attended = (accum / total).T
    for g in range(heads):
        at_own[:, g * HD : (g + 1) * HD] = attended[g * piece : (g + 1) * piece, :].astype(BF16)

    def at_copy(i, d):
        up = tree_a.up(d)
        span = pl.ds(i * piece, piece)
        src = at_own if up == 0 else at_in.at[up, span]
        return along_z(
            src, at_in.at[d, span], at_send.at[i, d], at_recv.at[i, d], DIRS[i], d - up
        )

    def forward_a(r):
        for i in (0, 1):
            if r:
                if r > tree_a.far(DIRS[i]):
                    continue
                at_copy(i, r).wait_recv()
            for d in tree_a.below(r, DIRS[i]):
                at_copy(i, d).start()

    def place(i, d):
        p = lax.rem(z - DIRS[i] * d + half + n, n)
        which = lax.div(p, m)
        owner = lax.rem(p, m)
        return which, owner, lax.rem(x - owner + m, m)

    def x_copy(i, d):
        which, owner, j = place(i, d)
        return pltpu.make_async_remote_copy(
            src_ref=x_out.at[i, d], dst_ref=x_in.at[which, j],
            send_sem=x_send.at[i, d], recv_sem=x_recv.at[which, j],
            device_id={"head": owner}, device_id_type=MESH,
        )

    def project(d):
        both = 0 < d < half
        a = at_own[...] if d == 0 else (at_in[d] if both else at_in[d, 0:piece, :])
        branch = jnp.dot(a, o_v[...], preferred_element_type=F32)
        for i in (0, 1) if both else (0,):
            term = branch[i * piece : (i + 1) * piece, :]
            which, owner, j = place(i, d)

            @pl.when(j == 0)
            def _():
                own_x[which] = term

            @pl.when(j != 0)
            def _():
                x_out[i, d] = term.astype(BF16)
                x_copy(i, d).start()

    def f_copy(which, j):
        p = x + which * m
        return pltpu.make_async_remote_copy(
            src_ref=fin.at[which], dst_ref=out_ref.at[rows_of(p)],
            send_sem=f_send.at[which, j], recv_sem=f_recv.at[which, j],
            device_id={"head": lax.rem(x + j, m)}, device_id_type=MESH,
        )

    strength = jnp.tanh(jnp.full((piece, depth), gate_ref[0], F32))

    def finish_rows(which):
        branch = own_x[which]
        for j in range(1, m):
            pltpu.make_async_remote_copy(
                src_ref=fin.at[0], dst_ref=x_in.at[which, j],
                send_sem=f_send.at[0, 0], recv_sem=x_recv.at[which, j],
                device_id={"head": lax.rem(x + j, m)}, device_id_type=MESH,
            ).wait_recv()
            branch = branch + x_in[which, j].astype(F32)
        p = x + which * m
        done = (text_v[rows_of(p), :].astype(F32) + strength * branch).astype(BF16)
        fin[which] = done
        for j in sorted(range(1, m), key=lambda j: -min(j, m - j)):
            f_copy(which, j).start()
        out_ref[rows_of(p), :] = done

    loads[4].wait()
    forward_a(0)
    forwarded = {0}
    early = lax.div(lax.rem(z + half - x + n + half // 2, n), half + 1)
    for d in range(half + 1):
        for r in (d, d + 1):
            if r in tree_a.relays and r not in forwarded:
                forward_a(r)
                forwarded.add(r)
        if d and d not in forwarded:
            for i in (0, 1):
                if d <= tree_a.far(DIRS[i]):
                    at_copy(i, d).wait_recv()
        project(d)
        if d == max(half // 2, half - 2):
            finish_rows(early)
    finish_rows(1 - early)

    for j in range(1, m):
        for which in (0, 1):
            p = lax.rem(x - j + m, m) + which * m
            pltpu.make_async_remote_copy(
                src_ref=fin.at[which], dst_ref=out_ref.at[rows_of(p)],
                send_sem=f_send.at[which, j], recv_sem=f_recv.at[which, j],
                device_id={"head": lax.rem(x + j, m)}, device_id_type=MESH,
            ).wait_recv()

    for i in (0, 1):
        for d in range(1, tree_p.far(DIRS[i]) + 1):
            ps_copy(i, d).wait_send()
            q_copy(i, d).wait_send()
            st_copy(i, d).wait_send()
            at_copy(i, d).wait_send()
        for d in range(0, half + 1):
            if i == 1 and d in (0, half):
                continue
            _, _, j = place(i, d)

            @pl.when(j != 0)
            def _():
                x_copy(i, d).wait_send()

    for which in (0, 1):
        for j in range(1, m):
            f_copy(which, j).wait_send()


STEPS = (3, 2, 3, 2)
BLOCK = 256


def body(text, q_weight, out_weight, keys, values, gate):
    n, m = lax.axis_size("tok"), lax.axis_size("head")
    half = n // 2
    assert n == 2 * m and keys.shape[1] == HD
    rows, depth = text.shape
    wide = q_weight.shape[1]
    tokens = keys.shape[0]
    piece = rows // n
    heads = wide // HD
    nq = heads * piece
    block = min(BLOCK, tokens)
    trees = tuple(Tree(half, s) for s in STEPS)
    vm, dma = pltpu.VMEM, pltpu.SemaphoreType.DMA
    slots = (2, half + 1)
    scratch = [
        vm((rows, depth), BF16), vm((depth, wide), BF16), vm((wide, depth), BF16),
        vm((tokens, HD), BF16), vm((tokens, HD), BF16), vm((HD, tokens), BF16), dma((5,)),
        vm((tokens, 2 * nq), F32),
        vm((rows, wide + HD), F32),
        vm((*slots, piece, wide + HD), BF16), vm((*slots, piece, wide + HD), BF16), dma(slots), dma(slots),
        vm((nq, HD), BF16), vm((half + 1, 2 * nq, HD), BF16), dma(slots), dma(slots),
        vm((*slots, HD, nq), F32), vm((*slots, 8, nq), F32),
        vm((*slots, HD + 16, nq), BF16), vm((*slots, HD + 16, nq), BF16), dma(slots), dma(slots),
        vm((piece, wide), BF16), vm((half + 1, 2 * piece, wide), BF16), dma(slots), dma(slots),
        vm((2, piece, depth), F32), vm((*slots, piece, depth), BF16), vm((2, m, piece, depth), BF16),
        dma(slots), dma((2, m)),
        vm((2, piece, depth), BF16), dma((2, m)), dma((2, m)),
    ]
    hbm = pl.BlockSpec(memory_space=pl.ANY)
    return pl.pallas_call(
        functools.partial(kernel, (n, m, half, trees, block)),
        out_shape=jax.ShapeDtypeStruct((rows, depth), BF16),
        in_specs=[hbm] * 5 + [pl.BlockSpec(memory_space=pltpu.SMEM)],
        out_specs=pl.BlockSpec(memory_space=pltpu.VMEM),
        scratch_shapes=scratch,
        compiler_params=pltpu.CompilerParams(
            collective_id=0, has_side_effects=True, vmem_limit_bytes=67043328
        ),
    )(text, q_weight, out_weight, keys, values, gate)


def solution(mesh):
    in_specs = (
        P(("groups", "row"), "tok"),
        P("tok", "head"),
        P("head", "tok"),
        P(("groups", "tok"), "head"),
        P(("groups", "tok"), "head"),
        P(),
    )
    out_specs = P(("groups", "row"), "tok")
    return jax.shard_map(body, mesh=mesh, in_specs=in_specs, out_specs=out_specs, check_vma=False)
```
